32 devices in a mesh: event: 2 (over x), draw: 8 (over z, y), bin: 2 (over core).
Axes of the slice: x: 2, y: 2, z: 4, core: 2. Of those that a mesh axis runs over, the one named last changes fastest.
Arguments:
- fine_cross: float32 [6, 2, 8192], P('event', None, 'draw'), parts along dimension 0, may hold values from -0.15 to 0.15
- fine_power: float32 [6, 8192], P('event', 'draw'), parts along dimension 0, may hold values from 0.000125 to 0.005
- bin_widths: int32 [256], P('event'), parts along dimension 0, may hold values from 1 to 128, 8192 in all
- log_amps: float32 [6, 8192], P('event', 'draw'), parts along dimension 0, may hold values from -0.5 to 0.5
- delays: float32 [6, 8192], P('event', 'draw'), parts along dimension 0, may hold values from -1.5 to 1.5
- phases: float32 [16384], P(('event', 'draw')), parts along dimension 0, may hold values from -3.140625 to 3.140625
- chirps: float32 [16384], P(('event', 'draw')), parts along dimension 0, may hold values from -8 to 8
- proposal_log: float32 [16384], P(('event', 'draw')), parts along dimension 0, may hold values from -100 to 130
Outputs:
- log_weights: float32 [16384], P(('event', 'draw')), parts along dimension 0
- log_evidence: float32 [2], P('event'), parts along dimension 0
The draws below stay inside these ranges and needn't reach their ends.
There are 2 independent parts, one for each index of `event`. The reference program is written for one: setup_inputs(seed, part) draws one part's arguments, and reference() takes and returns one part's arrays. A program takes and returns all parts, laid end to end along the dimension named above; each array names one. Nothing has to cross between parts.
Inputs may be any that keep to these rules, and one draw needn't show every extreme that they name: `bin_widths`: the widths of an event sum to 8192; each is 1 to 128 and one is exactly 128.
All inputs are finite; a program needn't handle non-finite values.
Results may differ from the reference program's by a relative error of at most 0.00016.
Values sent between devices are 32-bit elements; how exact they have to be, the bound alone decides.
A program may use at most 64 MiB of HBM per device.

```python
import math
import jax
import jax.numpy as jnp
import numpy as np
from jax import lax

DET = 3
BINS = 128
FINE = 8192
MOST_FINE = 128
TSHIFT = 2048
DRAWS = 8192


def draw_proposal_log(key, part):
    values = jax.random.normal(jax.random.fold_in(key, 72), (DRAWS,), jnp.float32)
    return jnp.clip(values, -3.0, 3.0)


def levels(key, extent, cuts, smallest, high):
    level, own = 1.0, jax.random.fold_in(key, 6)
    for dim, blocks in cuts:
        draws = jnp.exp(jax.random.uniform(jax.random.fold_in(own, dim), (blocks,), jnp.float32, smallest / len(cuts), high / len(cuts)))
        level = level * jnp.repeat(draws, extent[dim] // blocks).reshape([-1 if axis == dim else 1 for axis in range(len(extent))])
    return level


def profile(count, total, bound, skew):
    loads = [(1 << 20) // math.isqrt(standing ** skew) + 1 for standing in range(2, count + 1)]
    rest, given = total - bound - (count - 1), [1] * (count - 1)
    while rest > 0:
        free = [i for i in range(count - 1) if given[i] < bound]
        mass, budget = sum([loads[i] for i in free]), rest
        for i in free:
            extra = min(bound - given[i], max(1, budget * loads[i] // mass), rest)
            given[i] = given[i] + extra
            rest = rest - extra
    return np.array([bound] + given)


def ragged(stream_key, amount, total, reach, lean):
    if amount == 2:
        one = jax.random.randint(stream_key, (), max(1, total - reach), min(reach, total - 1) + 1)
        return jnp.stack([one, total - one])
    lengths = jnp.asarray(profile(amount, total, reach, lean), jnp.int32)
    pairs = (amount - 1) // 2
    giver, sink = lengths[1:1 + 2 * pairs:2], lengths[2:2 + 2 * pairs:2]
    room = jnp.minimum(giver - 1, reach - sink)
    shifted = jax.random.randint(jax.random.fold_in(stream_key, 1), (pairs,), 0, 1 << 20) % (room + 1)
    lengths = lengths.at[1:1 + 2 * pairs:2].set(giver - shifted).at[2:2 + 2 * pairs:2].set(sink + shifted)
    return lengths[jax.random.permutation(jax.random.fold_in(stream_key, 2), amount)]


def noise(key, dims, width, limit, cuts=(), kind=jnp.bfloat16):
    drawn = jax.random.normal(key, dims, jnp.float32) * width
    if len(cuts) > 0:
        drawn = levels(key, dims, cuts, -0.22, 0.18) * drawn
    return jnp.clip(drawn, min=-limit, max=limit).astype(kind)


def setup_inputs(seed: int = 0, part: int = 0) -> dict:
    arg_keys = jax.random.split(jax.random.key(seed), 9)
    part_keys = jax.random.split(jax.random.fold_in(arg_keys[8], part), 9)
    return {
        "fine_cross": noise(part_keys[0], (DET, 2, FINE), 0.025, 0.15, ((2, 8),), jnp.float32),
        "fine_power": jnp.clip(jnp.exp(math.log(0.005) - 3.6888794 * jax.random.uniform(part_keys[1], (DET, FINE), jnp.float32) ** levels(part_keys[1], (DET, FINE), ((1, 8),), -0.2, 0.2)), 0.000125, 0.005),
        "bin_widths": ragged(part_keys[2], BINS, FINE, MOST_FINE, 1).astype(jnp.int32),
        "log_amps": noise(part_keys[3], (DET, DRAWS), 0.1, 0.5, ((1, 8),), jnp.float32),
        "delays": noise(part_keys[4], (DET, DRAWS), 0.3, 1.5, ((1, 8),), jnp.float32),
        "phases": jnp.clip(jax.random.uniform(part_keys[5], (DRAWS,), jnp.float32, -3.140625, 3.140625), -3.140625, 3.140625),
        "chirps": noise(part_keys[6], (DRAWS,), 2.0, 8.0, ((0, 8),), jnp.float32),
        "proposal_log": draw_proposal_log(jax.random.fold_in(jax.random.fold_in(arg_keys[8], part), 71), part),
    }


TWO_PI = 2.0 * math.pi
TIME_STEP = 0.125
PRECISE = lax.Precision.HIGHEST


def summary_terms(cross_rows, power_rows, first_fine, lower_edge, bin_widths):
    fine_index = first_fine + jnp.arange(power_rows.shape[1], dtype=jnp.int32)
    upper_edge = lower_edge + bin_widths
    inside = ((fine_index[:, None] >= lower_edge[None, :]) & (fine_index[:, None] < upper_edge[None, :])).astype(jnp.float32)
    offset = fine_index.astype(jnp.float32)[:, None] + 0.5 - lower_edge.astype(jnp.float32)[None, :]
    weight = inside * offset / bin_widths.astype(jnp.float32)[None, :]
    lower_weight = inside - weight
    detectors = power_rows.shape[0]
    flattened = cross_rows.reshape(detectors * 2, -1)
    start_sums = jnp.dot(flattened, lower_weight, precision=PRECISE).reshape(detectors, 2, -1)
    end_sums = jnp.dot(flattened, weight, precision=PRECISE).reshape(detectors, 2, -1)
    power_low = jnp.dot(power_rows, lower_weight * lower_weight, precision=PRECISE)
    power_mixed = jnp.dot(power_rows, lower_weight * weight, precision=PRECISE)
    power_high = jnp.dot(power_rows, weight * weight, precision=PRECISE)
    return start_sums, end_sums, power_low, power_mixed, power_high


def edge_phase(freq_values, delays, phases, chirps):
    return ((TWO_PI * freq_values)[None, :, None] * delays[:, None, :] + phases[None, None, :]
            + chirps[None, None, :] * (freq_values * freq_values)[None, :, None])


def sample_terms(freq_low, freq_high, log_amps, delays, phases, chirps, power_low, power_mixed, power_high):
    amplitude = jnp.exp(log_amps)[:, None, :]
    phase_low = edge_phase(freq_low, delays, phases, chirps)
    phase_high = edge_phase(freq_high, delays, phases, chirps)
    pair_low = jnp.stack([amplitude * jnp.cos(phase_low), amplitude * jnp.sin(phase_low)], axis=2)
    pair_high = jnp.stack([amplitude * jnp.cos(phase_high), amplitude * jnp.sin(phase_high)], axis=2)
    features = jnp.stack([pair_low, pair_high], axis=2).reshape(-1, log_amps.shape[1])
    cos_diff = jnp.cos(phase_low - phase_high)
    inner_sum = jnp.sum(power_low + power_high, axis=1)[:, None] + 2.0 * jnp.einsum(
        'db,dbn->dn', power_mixed, cos_diff, precision=PRECISE)
    self_power = jnp.sum(jnp.exp(2.0 * log_amps) * inner_sum, axis=0)
    return features, self_power


def build_table(first_shift, row_count, total_shifts, start_sums, end_sums, freq_low, freq_high):
    shifts = (first_shift + jnp.arange(row_count, dtype=jnp.int32) - total_shifts // 2).astype(jnp.float32) * TIME_STEP
    edge_freq = jnp.stack([freq_low, freq_high], axis=-1)
    angles = (TWO_PI * edge_freq)[None] * shifts[:, None, None]
    cosine = jnp.cos(angles)[:, None]
    sine_value = jnp.sin(angles)[:, None]
    real_part = jnp.stack([start_sums[:, 0], end_sums[:, 0]], axis=-1)[None]
    imag_part = jnp.stack([start_sums[:, 1], end_sums[:, 1]], axis=-1)[None]
    table_real = real_part * cosine + imag_part * sine_value
    table_imag = imag_part * cosine - real_part * sine_value
    return jnp.stack([table_real, table_imag], axis=-1).reshape(row_count, -1)


def reference(fine_cross, fine_power, bin_widths, log_amps, delays, phases, chirps, proposal_log):
    upper_edge = jnp.cumsum(bin_widths).astype(jnp.int32)
    lower_edge = (upper_edge - bin_widths).astype(jnp.int32)
    start_sums, end_sums, power_low, power_mixed, power_high = summary_terms(
        fine_cross, fine_power, jnp.int32(0), lower_edge, bin_widths)
    freq_low = lower_edge.astype(jnp.float32) / FINE
    freq_high = upper_edge.astype(jnp.float32) / FINE
    features, self_power = sample_terms(freq_low, freq_high, log_amps, delays, phases, chirps,
                                        power_low, power_mixed, power_high)
    matrix = build_table(jnp.int32(0), TSHIFT, TSHIFT, start_sums, end_sums, freq_low, freq_high)
    cross_terms = jnp.dot(matrix, features, precision=PRECISE)
    scores = cross_terms - 0.5 * self_power[None, :] + proposal_log[None, :]
    largest = jnp.max(scores, axis=0)
    marginal = largest + jnp.log(jnp.sum(jnp.exp(scores - largest[None, :]), axis=0)) - math.log(TSHIFT)
    peak_value = jnp.max(marginal)
    total_log = peak_value + jnp.log(jnp.sum(jnp.exp(marginal - peak_value)))
    return marginal - total_log, (total_log - math.log(DRAWS)).reshape(1)
```

```python
import functools
import math

import jax
import jax.numpy as jnp
import numpy as np
from jax import lax
from jax.experimental import pallas as pl
from jax.experimental.pallas import tpu as pltpu
from jax.sharding import PartitionSpec as P

TSHIFT = 2048
STEPS_PER_UNIT = 8
LOG2E = math.log2(math.e)
LN2 = math.log(2.0)
LANES = 128
ROWS = 16
CHUNK = 128
F32 = jnp.float32
BF16 = jnp.bfloat16


def even_fit(func, terms):
    nodes = 0.125 * (1.0 + np.cos(np.pi * (np.arange(64) + 0.5) / 64))
    values = func(np.sqrt(nodes))
    fit = np.polynomial.chebyshev.Chebyshev.fit(nodes, values, terms - 1, domain=[0.0, 0.25])
    return [float(c) for c in fit.convert(kind=np.polynomial.Polynomial).coef]


SIN_COEF = even_fit(lambda u: np.sin(np.pi * u) / u, 6)
COS_COEF = even_fit(lambda u: np.cos(np.pi * u), 6)


def horner(z, coefs):
    total = jnp.full_like(z, coefs[-1])
    for c in coefs[-2::-1]:
        total = total * z + c
    return total


def cos_sin_turns(t):
    u = t - jnp.round(t)
    z = u * u
    s = u * horner(z, SIN_COEF)
    c = horner(z, COS_COEF)
    return 1.0 - 2.0 * (s * s), 2.0 * (s * c)


def halves(x):
    hi = x.astype(BF16)
    lo = (x - hi.astype(F32)).astype(BF16)
    return hi, lo


def each(count, step):
    if count <= 16:
        for i in range(count):
            step(i)
    else:
        lax.fori_loop(0, count, lambda i, c: (step(i), c)[1], 0)


def kernel(n_draw, n_bin, cross_ref, power_ref, width_ref, amp_ref, delay_ref, phase_ref, chirp_ref, prop_ref,
           out_ref, evid_ref, sums, packets, ctab, stab, acos, asin, cdiff, zr, zi, xcol, coef, base_ref,
           send1, recv1, send2, recv2):
    n_all = n_draw * n_bin
    my_draw, my_bin = lax.axis_index("draw"), lax.axis_index("bin")
    me = my_draw * n_bin + my_bin
    dets = power_ref.shape[0]
    fine = power_ref.shape[1]
    bins = width_ref.shape[1]
    half = phase_ref.shape[1] // n_bin
    grid_fine = fine * n_draw
    turns = 1.0 / (grid_fine * STEPS_PER_UNIT * 2)

    barrier = pltpu.get_barrier_semaphore()

    def greet(r):
        other = lax.rem(me + 1 + r, n_all)
        pl.semaphore_signal(barrier, inc=1, device_id={"draw": other // n_bin, "bin": lax.rem(other, n_bin)},
                            device_id_type=pl.DeviceIdType.MESH)

    each(n_all - 1, greet)

    width_row = width_ref[...].astype(F32)
    row_id = lax.broadcasted_iota(jnp.int32, (bins, bins), 0)
    lane_id = lax.broadcasted_iota(jnp.int32, (bins, bins), 1)
    wide = jnp.broadcast_to(width_row, (bins, bins))
    lower = jnp.sum(jnp.where(lane_id < row_id, wide, 0.0), axis=1, keepdims=True)
    width = jnp.sum(jnp.where(lane_id == row_id, wide, 0.0), axis=1, keepdims=True)
    upper_row = jnp.sum(jnp.where(row_id <= lane_id, jnp.broadcast_to(width, (bins, bins)), 0.0), axis=0, keepdims=True)
    xcol[...] = jnp.broadcast_to((lower + width) * (1.0 / grid_fine), (bins, LANES))

    first = (my_draw * fine).astype(F32)
    pos = lax.broadcasted_iota(jnp.int32, (bins, fine), 1).astype(F32) + (first + 0.5)
    off = pos - lower
    inside = (off > 0.0) & (off < width)
    onehot = jnp.where(inside, 1.0, 0.0).astype(BF16)
    w = jnp.sum(jnp.where(inside, off * (1.0 / width), 0.0), axis=0, keepdims=True)
    v = 1.0 - w
    crosses = [cross_ref[d] for d in range(dets)]
    power = power_ref[...]
    data = jnp.concatenate([c * v for c in crosses] + [c * w for c in crosses] + [power * (w * v)]
                           + [jnp.zeros((ROWS - 5 * dets, fine), F32)], axis=0)
    d0 = data.astype(BF16)
    rest = data - d0.astype(F32)
    d1 = rest.astype(BF16)
    d2 = (rest - d1.astype(F32)).astype(BF16)
    parts = lax.dot_general(jnp.concatenate([d0, d1, d2], axis=0), onehot, (((1,), (1,)), ((), ())),
                            preferred_element_type=F32)
    local = parts[:ROWS] + (parts[ROWS:2 * ROWS] + parts[2 * ROWS:])
    flat = jnp.sum(power * (v * v + w * w), axis=1, keepdims=True)
    lane_row = lax.broadcasted_iota(jnp.int32, (1, bins), 1)
    ends = jnp.zeros((1, bins), F32)
    for d in range(dets):
        ends = jnp.where(lane_row == d, flat[d:d + 1], ends)
    sub16 = lax.broadcasted_iota(jnp.int32, (ROWS, bins), 0)
    sums[my_draw] = jnp.where(sub16 == ROWS - 1, ends, local)

    pl.semaphore_wait(barrier, n_all - 1)

    def sum_copy(slot, dev):
        return pltpu.make_async_remote_copy(
            src_ref=sums.at[slot], dst_ref=sums.at[slot], send_sem=send1.at[dev], recv_sem=recv1.at[slot],
            device_id={"draw": dev, "bin": my_bin}, device_id_type=pl.DeviceIdType.MESH)

    each(n_draw - 1, lambda r: sum_copy(my_draw, lax.rem(my_draw + 1 + r, n_draw)).start())

    def table_rows(i, carry):
        at = pl.multiple_of(i * 16, 16)
        odd = (2 * (lax.broadcasted_iota(jnp.int32, (16, bins), 0) + at) + 1).astype(F32)
        c, s = cos_sin_turns(odd * upper_row * turns)
        ch, cl = halves(c)
        sh, sl = halves(s)
        ctab[pl.ds(at, 16), :] = jnp.concatenate([ch, ch, cl, cl], axis=1)
        stab[pl.ds(at, 16), :] = jnp.concatenate([sh, sh, sl, sl], axis=1)
        return carry

    lax.fori_loop(0, TSHIFT // 32, table_rows, 0)

    mine = pl.ds(pl.multiple_of(my_bin * half, half), half)
    amp = [jnp.exp(amp_ref[d:d + 1, mine]) for d in range(dets)]
    delay = [delay_ref[d:d + 1, mine] for d in range(dets)]
    phase = phase_ref[:, mine] * (1.0 / (2.0 * math.pi))
    chirp = chirp_ref[:, mine] * (1.0 / (2.0 * math.pi))
    cos0, sin0 = cos_sin_turns(phase)
    twice = [2.0 * a * a for a in amp]
    sub8 = lax.broadcasted_iota(jnp.int32, (8, half), 0)
    seeds = tuple(jnp.broadcast_to(x, (8, half)) for _ in range(dets) for x in (cos0, sin0))

    def feature_rows(i, carry):
        at = pl.multiple_of(i * 8, 8)
        x = xcol[pl.ds(at, 8), 0:1]
        shared = phase + chirp * (x * x)
        new = []
        for d in range(dets):
            c, s = cos_sin_turns(x * delay[d] + shared)
            cr, sr = pltpu.roll(c, 1, 0), pltpu.roll(s, 1, 0)
            cp = jnp.where(sub8 == 0, carry[2 * d], cr)
            sp = jnp.where(sub8 == 0, carry[2 * d + 1], sr)
            new += [cr, sr]
            cdiff[d, pl.ds(at, 8), :] = (c * cp + s * sp) * twice[d]
            acos[d, pl.ds(at, 8), :] = c * amp[d]
            asin[d, pl.ds(at, 8), :] = s * amp[d]
        return tuple(new)

    lax.fori_loop(0, bins // 8, feature_rows, seeds)

    each(n_draw - 1, lambda r: sum_copy(lax.rem(my_draw + 1 + r, n_draw), my_draw).wait_recv())
    total = sums[0]
    for i in range(1, n_draw):
        total = total + sums[i]

    start, end = total[:2 * dets], total[2 * dets:4 * dets]
    both = end + jnp.where(lane_row < bins - 1, pltpu.roll(total, bins - 1, 1)[:2 * dets], 0.0)
    rc, rs = cos_sin_turns(upper_row * turns)
    rc, rs = rc * LOG2E, rs * LOG2E
    rows = []
    for d in range(dets):
        re, im = both[2 * d:2 * d + 1], both[2 * d + 1:2 * d + 2]
        rows += [re * rc - im * rs, im * rc + re * rs]
    rows += [total[4 * dets + d:4 * dets + d + 1] for d in range(dets)]
    rows.append(jnp.zeros((LANES - len(rows), bins), F32))
    coef[...] = jnp.concatenate(rows, axis=0).T

    zero = jnp.zeros((8, half), F32)

    def mix_rows(i, power_sum):
        out_r, out_i = [], []
        for k in range(2):
            at = pl.multiple_of(i * 16 + 8 * k, 8)
            re = im = None
            for d in range(dets):
                ac, as_ = acos[d, pl.ds(at, 8), :], asin[d, pl.ds(at, 8), :]
                cr, ci = coef[pl.ds(at, 8), 2 * d:2 * d + 1], coef[pl.ds(at, 8), 2 * d + 1:2 * d + 2]
                r, m = cr * ac + ci * as_, ci * ac - cr * as_
                re, im = (r, m) if re is None else (re + r, im + m)
                pm = coef[pl.ds(at, 8), 2 * dets + d:2 * dets + d + 1]
                power_sum = power_sum + pm * cdiff[d, pl.ds(at, 8), :]
            out_r.append(re)
            out_i.append(im)
        for ref, val in ((zr, out_r), (zi, out_i)):
            hi, lo = halves(jnp.concatenate(val, axis=0))
            for part, block in enumerate((hi, lo, hi, lo)):
                ref[pl.ds(pl.multiple_of(part * bins + i * 16, 16), 16), :] = block
        return power_sum

    self_power = jnp.sum(lax.fori_loop(0, bins // 16, mix_rows, zero), axis=0, keepdims=True)
    fixed = jnp.zeros((1, half), F32)
    for d in range(dets):
        self_power = self_power + (0.5 * twice[d]) * total[ROWS - 1:ROWS, d:d + 1]
        fixed = fixed + amp[d] * (start[2 * d:2 * d + 1, 0:1] * cos0 + start[2 * d + 1:2 * d + 2, 0:1] * sin0)
    base_ref[...] = fixed - 0.5 * self_power + prop_ref[:, mine] - math.log(TSHIFT)

    top = jnp.full((8, half), -jnp.inf, F32)
    acc = zero
    for i in range(TSHIFT // 2 // CHUNK):
        a = jnp.dot(ctab[i * CHUNK:(i + 1) * CHUNK, :], zr[...], preferred_element_type=F32)
        b = jnp.dot(stab[i * CHUNK:(i + 1) * CHUNK, :], zi[...], preferred_element_type=F32)
        a = a.reshape(CHUNK // 8, 8, half)
        b = b.reshape(CHUNK // 8, 8, half)
        p, q = a + b, a - b
        new = jnp.maximum(top, jnp.max(jnp.maximum(p, q), axis=0))
        acc = acc * jnp.exp2(top - new) + jnp.sum(jnp.exp2(p - new[None]) + jnp.exp2(q - new[None]), axis=0)
        top = new
    peak = jnp.max(top, axis=0, keepdims=True)
    mass = jnp.sum(acc * jnp.exp2(top - peak), axis=0, keepdims=True)
    marginal = peak * LN2 + jnp.log(mass) + base_ref[...]

    largest = jnp.max(marginal, axis=1, keepdims=True)
    scaled = jnp.sum(jnp.exp(marginal - largest), axis=1, keepdims=True)
    count = half // LANES
    used = [marginal[:, i * LANES:(i + 1) * LANES] for i in range(count)]
    used += [jnp.broadcast_to(largest, (1, LANES)), jnp.broadcast_to(scaled, (1, LANES))]
    pad = packets.shape[1] - len(used)
    packets[me] = jnp.concatenate(used + [jnp.zeros((pad, LANES), F32)], axis=0)

    def packet_copy(slot, dev):
        return pltpu.make_async_remote_copy(
            src_ref=packets.at[slot], dst_ref=packets.at[slot], send_sem=send2.at[dev], recv_sem=recv2.at[slot],
            device_id={"draw": dev // n_bin, "bin": lax.rem(dev, n_bin)}, device_id_type=pl.DeviceIdType.MESH)

    each(n_all - 1, lambda r: packet_copy(me, lax.rem(me + 1 + r, n_all)).start())
    each(n_all - 1, lambda r: packet_copy(lax.rem(me + 1 + r, n_all), me).wait_recv())

    tops = packets[:, count, :]
    masses = packets[:, count + 1, :]
    whole_top = jnp.max(tops, axis=0, keepdims=True)
    whole = jnp.sum(masses * jnp.exp(tops - whole_top), axis=0, keepdims=True)
    total_log = whole_top + jnp.log(whole)
    for q in range(n_bin):
        out_ref[q * count:(q + 1) * count, :] = packets[my_draw * n_bin + q, 0:count, :] - total_log
    evid_ref[...] = total_log[:, 0:1] - math.log(half * n_all)

    each(n_draw - 1, lambda r: sum_copy(my_draw, lax.rem(my_draw + 1 + r, n_draw)).wait_send())
    each(n_all - 1, lambda r: packet_copy(me, lax.rem(me + 1 + r, n_all)).wait_send())


def body(n_draw, n_bin, fine_cross, fine_power, bin_widths, log_amps, delays, phases, chirps, proposal_log):
    dets = fine_power.shape[0]
    bins = bin_widths.shape[0]
    draws = phases.shape[0]
    half = draws // n_bin
    n_all = n_draw * n_bin
    packet_rows = -(-(half // LANES + 2) // 8) * 8
    vmem = pl.BlockSpec(memory_space=pltpu.VMEM)
    weights, evidence = pl.pallas_call(
        functools.partial(kernel, n_draw, n_bin),
        out_shape=(jax.ShapeDtypeStruct((draws // LANES, LANES), F32), jax.ShapeDtypeStruct((1, 1), F32)),
        in_specs=[vmem] * 8,
        out_specs=(vmem, vmem),
        scratch_shapes=[
            pltpu.VMEM((n_draw, ROWS, bins), F32),
            pltpu.VMEM((n_all, packet_rows, LANES), F32),
            pltpu.VMEM((TSHIFT // 2, 4 * bins), BF16),
            pltpu.VMEM((TSHIFT // 2, 4 * bins), BF16),
            pltpu.VMEM((dets, bins, half), F32),
            pltpu.VMEM((dets, bins, half), F32),
            pltpu.VMEM((dets, bins, half), F32),
            pltpu.VMEM((4 * bins, half), BF16),
            pltpu.VMEM((4 * bins, half), BF16),
            pltpu.VMEM((bins, LANES), F32),
            pltpu.VMEM((bins, LANES), F32),
            pltpu.VMEM((1, half), F32),
            pltpu.SemaphoreType.DMA((n_draw,)),
            pltpu.SemaphoreType.DMA((n_draw,)),
            pltpu.SemaphoreType.DMA((n_all,)),
            pltpu.SemaphoreType.DMA((n_all,)),
        ],
        compiler_params=pltpu.CompilerParams(collective_id=0, has_side_effects=True),
        name="evidence",
    )(fine_cross, fine_power, bin_widths.reshape(1, bins), log_amps, delays, phases.reshape(1, draws),
      chirps.reshape(1, draws), proposal_log.reshape(1, draws))
    return weights.reshape(draws), evidence.reshape(1)


def solution(mesh):
    placed = (
        P("event", None, "draw"),
        P("event", "draw"),
        P("event"),
        P("event", "draw"),
        P("event", "draw"),
        P(("event", "draw")),
        P(("event", "draw")),
        P(("event", "draw")),
    )
    return jax.shard_map(
        functools.partial(body, mesh.shape["draw"], mesh.shape["bin"]),
        mesh=mesh,
        in_specs=placed,
        out_specs=(P(("event", "draw")), P("event")),
        check_vma=False,
    )
```

```python
import functools
import math

import jax
import jax.numpy as jnp
import numpy as np
from jax import lax
from jax.experimental import pallas as pl
from jax.experimental.pallas import tpu as pltpu
from jax.sharding import PartitionSpec as P

TSHIFT = 2048
STEPS_PER_UNIT = 8
LOG2E = math.log2(math.e)
LN2 = math.log(2.0)
LANES = 128
ROWS = 16
CHUNK = 128
F32 = jnp.float32
BF16 = jnp.bfloat16


def even_fit(func, terms):
    nodes = 0.125 * (1.0 + np.cos(np.pi * (np.arange(64) + 0.5) / 64))
    values = func(np.sqrt(nodes))
    fit = np.polynomial.chebyshev.Chebyshev.fit(nodes, values, terms - 1, domain=[0.0, 0.25])
    return [float(c) for c in fit.convert(kind=np.polynomial.Polynomial).coef]


SIN_COEF = even_fit(lambda u: np.sin(np.pi * u) / u, 6)
COS_COEF = even_fit(lambda u: np.cos(np.pi * u), 6)


def horner(z, coefs):
    total = jnp.full_like(z, coefs[-1])
    for c in coefs[-2::-1]:
        total = total * z + c
    return total


def cos_sin_turns(t):
    u = t - jnp.round(t)
    z = u * u
    s = u * horner(z, SIN_COEF)
    c = horner(z, COS_COEF)
    return 1.0 - 2.0 * (s * s), 2.0 * (s * c)


def halves(x):
    hi = x.astype(BF16)
    lo = (x - hi.astype(F32)).astype(BF16)
    return hi, lo


def each(count, step):
    if count <= 16:
        for i in range(count):
            step(i)
    else:
        lax.fori_loop(0, count, lambda i, c: (step(i), c)[1], 0)


def kernel(n_draw, n_bin, cross_in, power_in, width_in, amp_in, delay_in, phase_in, chirp_in, prop_in,
           out_ref, evid_ref, cross_ref, power_ref, width_ref, amp_ref, delay_ref, phase_ref, chirp_ref, prop_ref,
           sums, stats, margs, ctab, stab, acos, asin, cdiff, zr, zi, xcol, coef, base_ref,
           load_sem, send1, recv1, send2, recv2, send3, recv3):
    loads = [pltpu.make_async_copy(src, dst, load_sem.at[i]) for i, (src, dst) in enumerate((
        (width_in, width_ref), (cross_in, cross_ref), (power_in, power_ref), (amp_in, amp_ref), (delay_in, delay_ref),
        (phase_in, phase_ref), (chirp_in, chirp_ref), (prop_in, prop_ref)))]
    for load in loads:
        load.start()
    n_all = n_draw * n_bin
    my_draw, my_bin = lax.axis_index("draw"), lax.axis_index("bin")
    me = my_draw * n_bin + my_bin
    dets = power_ref.shape[0]
    fine = power_ref.shape[1]
    bins = width_ref.shape[1]
    half = phase_ref.shape[1] // n_bin
    grid_fine = fine * n_draw
    turns = 1.0 / (grid_fine * STEPS_PER_UNIT * 2)

    barrier = pltpu.get_barrier_semaphore()

    def greet(r):
        other = lax.rem(me + 1 + r, n_all)
        pl.semaphore_signal(barrier, inc=1, device_id={"draw": other // n_bin, "bin": lax.rem(other, n_bin)},
                            device_id_type=pl.DeviceIdType.MESH)

    each(n_all - 1, greet)

    for load in loads[:3]:
        load.wait()

    width_row = width_ref[...].astype(F32)
    row_id = lax.broadcasted_iota(jnp.int32, (bins, bins), 0)
    lane_id = lax.broadcasted_iota(jnp.int32, (bins, bins), 1)
    wide = jnp.broadcast_to(width_row, (bins, bins))
    lower = jnp.sum(jnp.where(lane_id < row_id, wide, 0.0), axis=1, keepdims=True)
    width = jnp.sum(jnp.where(lane_id == row_id, wide, 0.0), axis=1, keepdims=True)
    upper_row = jnp.sum(jnp.where(row_id <= lane_id, jnp.broadcast_to(width, (bins, bins)), 0.0), axis=0, keepdims=True)
    xcol[...] = jnp.broadcast_to((lower + width) * (1.0 / grid_fine), (bins, LANES))

    def table_rows(i, carry):
        at = pl.multiple_of(i * 16, 16)
        odd = (2 * (lax.broadcasted_iota(jnp.int32, (16, bins), 0) + at) + 1).astype(F32)
        c, s = cos_sin_turns(odd * upper_row * turns)
        ch, cl = halves(c)
        sh, sl = halves(s)
        ctab[pl.ds(at, 16), :] = jnp.concatenate([ch, ch, cl, cl], axis=1)
        stab[pl.ds(at, 16), :] = jnp.concatenate([sh, sh, sl, sl], axis=1)
        return carry

    first = (my_draw * fine).astype(F32)
    pos = lax.broadcasted_iota(jnp.int32, (bins, fine), 1).astype(F32) + (first + 0.5)
    off = pos - lower
    inside = (off > 0.0) & (off < width)
    onehot = jnp.where(inside, 1.0, 0.0).astype(BF16)
    w = jnp.sum(jnp.where(inside, off * (1.0 / width), 0.0), axis=0, keepdims=True)
    v = 1.0 - w
    crosses = [cross_ref[d] for d in range(dets)]
    power = power_ref[...]
    data = jnp.concatenate([c * v for c in crosses] + [c * w for c in crosses] + [power * (w * v)]
                           + [jnp.zeros((ROWS - 5 * dets, fine), F32)], axis=0)
    d0 = data.astype(BF16)
    rest = data - d0.astype(F32)
    d1 = rest.astype(BF16)
    d2 = (rest - d1.astype(F32)).astype(BF16)
    parts = lax.dot_general(jnp.concatenate([d0, d1, d2], axis=0), onehot, (((1,), (1,)), ((), ())),
                            preferred_element_type=F32)
    local = parts[:ROWS] + (parts[ROWS:2 * ROWS] + parts[2 * ROWS:])
    lane_row = lax.broadcasted_iota(jnp.int32, (1, bins), 1)
    start, end = local[:2 * dets], local[2 * dets:4 * dets]
    both = end + jnp.where(lane_row < bins - 1, pltpu.roll(local, bins - 1, 1)[:2 * dets], 0.0)
    flat = jnp.sum(power * (v * v + w * w), axis=1, keepdims=True)
    ends = jnp.zeros((1, bins), F32)
    for d in range(dets):
        ends = jnp.where(lane_row == d, flat[d:d + 1], ends)
    for r in range(2 * dets):
        ends = jnp.where(lane_row == dets + r, start[r:r + 1, 0:1], ends)
    packed = [both, local[4 * dets:5 * dets], ends]
    sums[my_draw] = jnp.concatenate(packed, axis=0)

    lax.fori_loop(0, TSHIFT // 64, table_rows, 0)
    pl.semaphore_wait(barrier, n_all - 1)

    def sum_copy(slot, dev):
        return pltpu.make_async_remote_copy(
            src_ref=sums.at[slot], dst_ref=sums.at[slot], send_sem=send1.at[dev], recv_sem=recv1.at[slot],
            device_id={"draw": dev, "bin": my_bin}, device_id_type=pl.DeviceIdType.MESH)

    each(n_draw - 1, lambda r: sum_copy(my_draw, lax.rem(my_draw + 1 + r, n_draw)).start())

    lax.fori_loop(TSHIFT // 64, TSHIFT // 32, table_rows, 0)
    for load in loads[3:]:
        load.wait()
    mine = pl.ds(pl.multiple_of(my_bin * half, half), half)
    amp = [jnp.exp(amp_ref[d:d + 1, mine]) for d in range(dets)]
    delay = [delay_ref[d:d + 1, mine] for d in range(dets)]
    phase = phase_ref[:, mine] * (1.0 / (2.0 * math.pi))
    chirp = chirp_ref[:, mine] * (1.0 / (2.0 * math.pi))
    cos0, sin0 = cos_sin_turns(phase)
    twice = [2.0 * a * a for a in amp]
    sub8 = lax.broadcasted_iota(jnp.int32, (8, half), 0)
    seeds = tuple(jnp.broadcast_to(x, (8, half)) for _ in range(dets) for x in (cos0, sin0))

    def feature_rows(i, carry):
        at = pl.multiple_of(i * 8, 8)
        x = xcol[pl.ds(at, 8), 0:1]
        shared = phase + chirp * (x * x)
        new = []
        for d in range(dets):
            c, s = cos_sin_turns(x * delay[d] + shared)
            cr, sr = pltpu.roll(c, 1, 0), pltpu.roll(s, 1, 0)
            cp = jnp.where(sub8 == 0, carry[2 * d], cr)
            sp = jnp.where(sub8 == 0, carry[2 * d + 1], sr)
            new += [cr, sr]
            cdiff[d, pl.ds(at, 8), :] = (c * cp + s * sp) * twice[d]
            acos[d, pl.ds(at, 8), :] = c * amp[d]
            asin[d, pl.ds(at, 8), :] = s * amp[d]
        return tuple(new)

    lax.fori_loop(0, bins // 8, feature_rows, seeds)

    each(n_draw - 1, lambda r: sum_copy(lax.rem(my_draw + 1 + r, n_draw), my_draw).wait_recv())
    total = sums[0]
    for i in range(1, n_draw):
        total = total + sums[i]

    rc, rs = cos_sin_turns(upper_row * turns)
    rc, rs = rc * LOG2E, rs * LOG2E
    rows = []
    for d in range(dets):
        re, im = total[2 * d:2 * d + 1], total[2 * d + 1:2 * d + 2]
        rows += [re * rc - im * rs, im * rc + re * rs]
    rows.append(total[2 * dets:3 * dets])
    rows.append(jnp.zeros((LANES - 3 * dets, bins), F32))
    coef[...] = jnp.concatenate(rows, axis=0).T

    zero = jnp.zeros((8, half), F32)

    def mix_rows(i, power_sum):
        out_r, out_i = [], []
        for k in range(2):
            at = pl.multiple_of(i * 16 + 8 * k, 8)
            re = im = None
            for d in range(dets):
                ac, as_ = acos[d, pl.ds(at, 8), :], asin[d, pl.ds(at, 8), :]
                cr, ci = coef[pl.ds(at, 8), 2 * d:2 * d + 1], coef[pl.ds(at, 8), 2 * d + 1:2 * d + 2]
                r, m = cr * ac + ci * as_, ci * ac - cr * as_
                re, im = (r, m) if re is None else (re + r, im + m)
                pm = coef[pl.ds(at, 8), 2 * dets + d:2 * dets + d + 1]
                power_sum = power_sum + pm * cdiff[d, pl.ds(at, 8), :]
            out_r.append(re)
            out_i.append(im)
        for ref, val in ((zr, out_r), (zi, out_i)):
            hi, lo = halves(jnp.concatenate(val, axis=0))
            for part, block in enumerate((hi, lo, hi, lo)):
                ref[pl.ds(pl.multiple_of(part * bins + i * 16, 16), 16), :] = block
        return power_sum

    self_power = jnp.sum(lax.fori_loop(0, bins // 16, mix_rows, zero), axis=0, keepdims=True)
    fixed = jnp.zeros((1, half), F32)
    misc = total[3 * dets:3 * dets + 1]
    for d in range(dets):
        self_power = self_power + (0.5 * twice[d]) * misc[:, d:d + 1]
        at = dets + 2 * d
        fixed = fixed + amp[d] * (misc[:, at:at + 1] * cos0 + misc[:, at + 1:at + 2] * sin0)
    base_ref[...] = fixed - 0.5 * self_power + prop_ref[:, mine] - math.log(TSHIFT)

    top = jnp.full((8, half), -jnp.inf, F32)
    acc = zero
    for i in range(TSHIFT // 2 // CHUNK):
        a = jnp.dot(ctab[i * CHUNK:(i + 1) * CHUNK, :], zr[...], preferred_element_type=F32)
        b = jnp.dot(stab[i * CHUNK:(i + 1) * CHUNK, :], zi[...], preferred_element_type=F32)
        a = a.reshape(CHUNK // 8, 8, half)
        b = b.reshape(CHUNK // 8, 8, half)
        p, q = a + b, a - b
        new = jnp.maximum(top, jnp.max(jnp.maximum(p, q), axis=0))
        acc = acc * jnp.exp2(top - new) + jnp.sum(jnp.exp2(p - new[None]) + jnp.exp2(q - new[None]), axis=0)
        top = new
    peak = jnp.max(top, axis=0, keepdims=True)
    mass = jnp.sum(acc * jnp.exp2(top - peak), axis=0, keepdims=True)
    marginal = peak * LN2 + jnp.log(mass) + base_ref[...]

    largest = jnp.max(marginal, axis=1, keepdims=True)
    scaled = jnp.sum(jnp.exp(marginal - largest), axis=1, keepdims=True)
    lane = lax.broadcasted_iota(jnp.int32, (1, LANES), 1)
    stats[me] = jnp.where(lane < LANES // 2, largest, scaled)
    margs[my_bin] = marginal

    def stat_copy(slot, dev):
        return pltpu.make_async_remote_copy(
            src_ref=stats.at[slot], dst_ref=stats.at[slot], send_sem=send2.at[dev], recv_sem=recv2.at[slot],
            device_id={"draw": dev // n_bin, "bin": lax.rem(dev, n_bin)}, device_id_type=pl.DeviceIdType.MESH)

    def marg_copy(slot, dev):
        return pltpu.make_async_remote_copy(
            src_ref=margs.at[slot], dst_ref=margs.at[slot], send_sem=send3.at[dev], recv_sem=recv3.at[slot],
            device_id={"draw": my_draw, "bin": dev}, device_id_type=pl.DeviceIdType.MESH)

    each(n_all - 1, lambda r: stat_copy(me, lax.rem(me + 1 + r, n_all)).start())
    each(n_bin - 1, lambda r: marg_copy(my_bin, lax.rem(my_bin + 1 + r, n_bin)).start())
    each(n_all - 1, lambda r: stat_copy(lax.rem(me + 1 + r, n_all), me).wait_recv())

    tops = [stats[i] for i in range(n_all)]
    whole_top = functools.reduce(jnp.maximum, tops)
    whole = functools.reduce(jnp.add, [pltpu.roll(x, LANES // 2, 1) * jnp.exp(x - whole_top) for x in tops])
    total_log = (whole_top + jnp.log(whole))[:, 0:1]
    evid_ref[...] = total_log - math.log(half * n_all)
    each(n_bin - 1, lambda r: marg_copy(lax.rem(my_bin + 1 + r, n_bin), my_bin).wait_recv())
    for q in range(n_bin):
        out_ref[:, q * half:(q + 1) * half] = margs[q] - total_log

    each(n_draw - 1, lambda r: sum_copy(my_draw, lax.rem(my_draw + 1 + r, n_draw)).wait_send())
    each(n_all - 1, lambda r: stat_copy(me, lax.rem(me + 1 + r, n_all)).wait_send())
    each(n_bin - 1, lambda r: marg_copy(my_bin, lax.rem(my_bin + 1 + r, n_bin)).wait_send())


def body(n_draw, n_bin, fine_cross, fine_power, bin_widths, log_amps, delays, phases, chirps, proposal_log):
    dets = fine_power.shape[0]
    bins = bin_widths.shape[0]
    draws = phases.shape[0]
    half = draws // n_bin
    n_all = n_draw * n_bin
    vmem = pl.BlockSpec(memory_space=pltpu.VMEM)
    weights, evidence = pl.pallas_call(
        functools.partial(kernel, n_draw, n_bin),
        out_shape=(pltpu.VMEM((1, draws), F32), jax.ShapeDtypeStruct((1, 1), F32)),
        in_specs=[pl.BlockSpec(memory_space=pltpu.HBM)] * 8,
        out_specs=(vmem, vmem),
        scratch_shapes=[
            pltpu.VMEM(fine_cross.shape, F32),
            pltpu.VMEM(fine_power.shape, F32),
            pltpu.VMEM((1, bins), jnp.int32),
            pltpu.VMEM(log_amps.shape, F32),
            pltpu.VMEM(delays.shape, F32),
            pltpu.VMEM((1, draws), F32),
            pltpu.VMEM((1, draws), F32),
            pltpu.VMEM((1, draws), F32),
            pltpu.VMEM((n_draw, 3 * dets + 1, bins), F32),
            pltpu.VMEM((n_all, 1, LANES), F32),
            pltpu.VMEM((n_bin, 1, half), F32),
            pltpu.VMEM((TSHIFT // 2, 4 * bins), BF16),
            pltpu.VMEM((TSHIFT // 2, 4 * bins), BF16),
            pltpu.VMEM((dets, bins, half), F32),
            pltpu.VMEM((dets, bins, half), F32),
            pltpu.VMEM((dets, bins, half), F32),
            pltpu.VMEM((4 * bins, half), BF16),
            pltpu.VMEM((4 * bins, half), BF16),
            pltpu.VMEM((bins, LANES), F32),
            pltpu.VMEM((bins, LANES), F32),
            pltpu.VMEM((1, half), F32),
            pltpu.SemaphoreType.DMA((8,)),
            pltpu.SemaphoreType.DMA((n_draw,)),
            pltpu.SemaphoreType.DMA((n_draw,)),
            pltpu.SemaphoreType.DMA((n_all,)),
            pltpu.SemaphoreType.DMA((n_all,)),
            pltpu.SemaphoreType.DMA((n_bin,)),
            pltpu.SemaphoreType.DMA((n_bin,)),
        ],
        compiler_params=pltpu.CompilerParams(collective_id=0, has_side_effects=True),
        name="evidence",
    )(fine_cross, fine_power, bin_widths.reshape(1, bins), log_amps, delays, phases.reshape(1, draws),
      chirps.reshape(1, draws), proposal_log.reshape(1, draws))
    return weights.reshape(draws), evidence.reshape(1)


def solution(mesh):
    placed = (
        P("event", None, "draw"),
        P("event", "draw"),
        P("event"),
        P("event", "draw"),
        P("event", "draw"),
        P(("event", "draw")),
        P(("event", "draw")),
        P(("event", "draw")),
    )
    return jax.shard_map(
        functools.partial(body, mesh.shape["draw"], mesh.shape["bin"]),
        mesh=mesh,
        in_specs=placed,
        out_specs=(P(("event", "draw")), P("event")),
        check_vma=False,
    )
```

```python
import functools
import math

import jax
import jax.numpy as jnp
import numpy as np
from jax import lax
from jax.experimental import pallas as pl
from jax.experimental.pallas import tpu as pltpu
from jax.sharding import PartitionSpec as P

TSHIFT = 2048
STEPS_PER_UNIT = 8
LOG2E = math.log2(math.e)
LN2 = math.log(2.0)
LANES = 128
ROWS = 16
CHUNK = 128
F32 = jnp.float32
BF16 = jnp.bfloat16


def even_fit(func, terms):
    nodes = 0.125 * (1.0 + np.cos(np.pi * (np.arange(64) + 0.5) / 64))
    values = func(np.sqrt(nodes))
    fit = np.polynomial.chebyshev.Chebyshev.fit(nodes, values, terms - 1, domain=[0.0, 0.25])
    return [float(c) for c in fit.convert(kind=np.polynomial.Polynomial).coef]


SIN_COEF = even_fit(lambda u: np.sin(np.pi * u) / u, 6)
COS_COEF = even_fit(lambda u: np.cos(np.pi * u), 6)


def horner(z, coefs):
    total = jnp.full_like(z, coefs[-1])
    for c in coefs[-2::-1]:
        total = total * z + c
    return total


def cos_sin_turns(t):
    u = t - jnp.round(t)
    z = u * u
    s = u * horner(z, SIN_COEF)
    c = horner(z, COS_COEF)
    return 1.0 - 2.0 * (s * s), 2.0 * (s * c)


def halves(x):
    hi = x.astype(BF16)
    lo = (x - hi.astype(F32)).astype(BF16)
    return hi, lo


def each(count, step):
    if count <= 16:
        for i in range(count):
            step(i)
    else:
        lax.fori_loop(0, count, lambda i, c: (step(i), c)[1], 0)


def kernel(n_draw, n_bin, cross_in, power_in, width_in, amp_in, delay_in, phase_in, chirp_in, prop_in,
           out_ref, cross_ref, power_ref, width_ref, amp_ref, delay_ref, phase_ref, chirp_ref, prop_ref,
           sums, stats, margs, ctab, stab, acos, asin, cdiff, zr, zi, xcol, coef, base_ref,
           load_sem, send1, recv1, send2, recv2, send3, recv3):
    loads = [pltpu.make_async_copy(src, dst, load_sem.at[i]) for i, (src, dst) in enumerate((
        (width_in, width_ref), (cross_in, cross_ref), (power_in, power_ref), (amp_in, amp_ref), (delay_in, delay_ref),
        (phase_in, phase_ref), (chirp_in, chirp_ref), (prop_in, prop_ref)))]
    for load in loads:
        load.start()
    n_all = n_draw * n_bin
    my_draw, my_bin = lax.axis_index("draw"), lax.axis_index("bin")
    me = my_draw * n_bin + my_bin
    dets = power_ref.shape[0]
    fine = power_ref.shape[1]
    bins = width_ref.shape[1]
    half = phase_ref.shape[1] // n_bin
    grid_fine = fine * n_draw
    turns = 1.0 / (grid_fine * STEPS_PER_UNIT * 2)

    barrier = pltpu.get_barrier_semaphore()

    def greet(r):
        other = lax.rem(me + 1 + r, n_all)
        pl.semaphore_signal(barrier, inc=1, device_id={"draw": other // n_bin, "bin": lax.rem(other, n_bin)},
                            device_id_type=pl.DeviceIdType.MESH)

    each(n_all - 1, greet)

    for load in loads[:3]:
        load.wait()

    width_row = width_ref[...].astype(F32)
    row_id = lax.broadcasted_iota(jnp.int32, (bins, bins), 0)
    lane_id = lax.broadcasted_iota(jnp.int32, (bins, bins), 1)
    wide = jnp.broadcast_to(width_row, (bins, bins))
    lower = jnp.sum(jnp.where(lane_id < row_id, wide, 0.0), axis=1, keepdims=True)
    width = jnp.sum(jnp.where(lane_id == row_id, wide, 0.0), axis=1, keepdims=True)
    upper_row = jnp.sum(jnp.where(row_id <= lane_id, jnp.broadcast_to(width, (bins, bins)), 0.0), axis=0, keepdims=True)
    xcol[...] = jnp.broadcast_to((lower + width) * (1.0 / grid_fine), (bins, LANES))

    def table_rows(i, carry):
        at = pl.multiple_of(i * 16, 16)
        odd = (2 * (lax.broadcasted_iota(jnp.int32, (16, bins), 0) + at) + 1).astype(F32)
        c, s = cos_sin_turns(odd * upper_row * turns)
        ch, cl = halves(c)
        sh, sl = halves(s)
        ctab[pl.ds(at, 16), :] = jnp.concatenate([ch, ch, cl, cl], axis=1)
        stab[pl.ds(at, 16), :] = jnp.concatenate([sh, sh, sl, sl], axis=1)
        return carry

    first = (my_draw * fine).astype(F32)
    pos = lax.broadcasted_iota(jnp.int32, (bins, fine), 1).astype(F32) + (first + 0.5)
    off = pos - lower
    inside = (off > 0.0) & (off < width)
    onehot = jnp.where(inside, 1.0, 0.0).astype(BF16)
    w = jnp.sum(jnp.where(inside, off * (1.0 / width), 0.0), axis=0, keepdims=True)
    v = 1.0 - w
    crosses = [cross_ref[d] for d in range(dets)]
    power = power_ref[...]
    data = jnp.concatenate([c * v for c in crosses] + [c * w for c in crosses] + [power * (w * v)]
                           + [jnp.zeros((ROWS - 5 * dets, fine), F32)], axis=0)
    d0 = data.astype(BF16)
    rest = data - d0.astype(F32)
    d1 = rest.astype(BF16)
    d2 = (rest - d1.astype(F32)).astype(BF16)
    parts = lax.dot_general(jnp.concatenate([d0, d1, d2], axis=0), onehot, (((1,), (1,)), ((), ())),
                            preferred_element_type=F32)
    local = parts[:ROWS] + (parts[ROWS:2 * ROWS] + parts[2 * ROWS:])
    lane_row = lax.broadcasted_iota(jnp.int32, (1, bins), 1)
    start, end = local[:2 * dets], local[2 * dets:4 * dets]
    both = end + jnp.where(lane_row < bins - 1, pltpu.roll(local, bins - 1, 1)[:2 * dets], 0.0)
    flat = jnp.sum(power * (v * v + w * w), axis=1, keepdims=True)
    ends = jnp.zeros((1, bins), F32)
    for d in range(dets):
        ends = jnp.where(lane_row == d, flat[d:d + 1], ends)
    for r in range(2 * dets):
        ends = jnp.where(lane_row == dets + r, start[r:r + 1, 0:1], ends)
    packed = [both, local[4 * dets:5 * dets], ends]
    sums[my_draw] = jnp.concatenate(packed, axis=0)

    lax.fori_loop(0, TSHIFT // 64, table_rows, 0)
    pl.semaphore_wait(barrier, n_all - 1)

    def sum_copy(slot, dev):
        return pltpu.make_async_remote_copy(
            src_ref=sums.at[slot], dst_ref=sums.at[slot], send_sem=send1.at[dev], recv_sem=recv1.at[slot],
            device_id={"draw": dev, "bin": my_bin}, device_id_type=pl.DeviceIdType.MESH)

    each(n_draw - 1, lambda r: sum_copy(my_draw, lax.rem(my_draw + 1 + r, n_draw)).start())

    lax.fori_loop(TSHIFT // 64, TSHIFT // 32, table_rows, 0)
    for load in loads[3:]:
        load.wait()
    mine = pl.ds(pl.multiple_of(my_bin * half, half), half)
    amp = [jnp.exp(amp_ref[d:d + 1, mine]) for d in range(dets)]
    delay = [delay_ref[d:d + 1, mine] for d in range(dets)]
    phase = phase_ref[:, mine] * (1.0 / (2.0 * math.pi))
    chirp = chirp_ref[:, mine] * (1.0 / (2.0 * math.pi))
    cos0, sin0 = cos_sin_turns(phase)
    twice = [2.0 * a * a for a in amp]
    sub8 = lax.broadcasted_iota(jnp.int32, (8, half), 0)
    seeds = tuple(jnp.broadcast_to(x, (8, half)) for _ in range(dets) for x in (cos0, sin0))

    def feature_rows(i, carry):
        at = pl.multiple_of(i * 8, 8)
        x = xcol[pl.ds(at, 8), 0:1]
        shared = phase + chirp * (x * x)
        new = []
        for d in range(dets):
            c, s = cos_sin_turns(x * delay[d] + shared)
            cr, sr = pltpu.roll(c, 1, 0), pltpu.roll(s, 1, 0)
            cp = jnp.where(sub8 == 0, carry[2 * d], cr)
            sp = jnp.where(sub8 == 0, carry[2 * d + 1], sr)
            new += [cr, sr]
            cdiff[d, pl.ds(at, 8), :] = (c * cp + s * sp) * twice[d]
            acos[d, pl.ds(at, 8), :] = c * amp[d]
            asin[d, pl.ds(at, 8), :] = s * amp[d]
        return tuple(new)

    lax.fori_loop(0, bins // 8, feature_rows, seeds)

    each(n_draw - 1, lambda r: sum_copy(lax.rem(my_draw + 1 + r, n_draw), my_draw).wait_recv())
    total = sums[0]
    for i in range(1, n_draw):
        total = total + sums[i]

    rc, rs = cos_sin_turns(upper_row * turns)
    rc, rs = rc * LOG2E, rs * LOG2E
    rows = []
    for d in range(dets):
        re, im = total[2 * d:2 * d + 1], total[2 * d + 1:2 * d + 2]
        rows += [re * rc - im * rs, im * rc + re * rs]
    rows.append(total[2 * dets:3 * dets])
    rows.append(jnp.zeros((LANES - 3 * dets, bins), F32))
    coef[...] = jnp.concatenate(rows, axis=0).T

    zero = jnp.zeros((8, half), F32)

    def mix_rows(i, power_sum):
        out_r, out_i = [], []
        for k in range(2):
            at = pl.multiple_of(i * 16 + 8 * k, 8)
            re = im = None
            for d in range(dets):
                ac, as_ = acos[d, pl.ds(at, 8), :], asin[d, pl.ds(at, 8), :]
                cr, ci = coef[pl.ds(at, 8), 2 * d:2 * d + 1], coef[pl.ds(at, 8), 2 * d + 1:2 * d + 2]
                r, m = cr * ac + ci * as_, ci * ac - cr * as_
                re, im = (r, m) if re is None else (re + r, im + m)
                pm = coef[pl.ds(at, 8), 2 * dets + d:2 * dets + d + 1]
                power_sum = power_sum + pm * cdiff[d, pl.ds(at, 8), :]
            out_r.append(re)
            out_i.append(im)
        for ref, val in ((zr, out_r), (zi, out_i)):
            hi, lo = halves(jnp.concatenate(val, axis=0))
            for part, block in enumerate((hi, lo, hi, lo)):
                ref[pl.ds(pl.multiple_of(part * bins + i * 16, 16), 16), :] = block
        return power_sum

    self_power = jnp.sum(lax.fori_loop(0, bins // 16, mix_rows, zero), axis=0, keepdims=True)
    fixed = jnp.zeros((1, half), F32)
    misc = total[3 * dets:3 * dets + 1]
    for d in range(dets):
        self_power = self_power + (0.5 * twice[d]) * misc[:, d:d + 1]
        at = dets + 2 * d
        fixed = fixed + amp[d] * (misc[:, at:at + 1] * cos0 + misc[:, at + 1:at + 2] * sin0)
    base_ref[...] = fixed - 0.5 * self_power + prop_ref[:, mine] - math.log(TSHIFT)

    top = jnp.full((8, half), -jnp.inf, F32)
    acc = zero
    for i in range(TSHIFT // 2 // CHUNK):
        a = jnp.dot(ctab[i * CHUNK:(i + 1) * CHUNK, :], zr[...], preferred_element_type=F32)
        b = jnp.dot(stab[i * CHUNK:(i + 1) * CHUNK, :], zi[...], preferred_element_type=F32)
        a = a.reshape(CHUNK // 8, 8, half)
        b = b.reshape(CHUNK // 8, 8, half)
        p, q = a + b, a - b
        new = jnp.maximum(top, jnp.max(jnp.maximum(p, q), axis=0))
        acc = acc * jnp.exp2(top - new) + jnp.sum(jnp.exp2(p - new[None]) + jnp.exp2(q - new[None]), axis=0)
        top = new
    peak = jnp.max(top, axis=0, keepdims=True)
    mass = jnp.sum(acc * jnp.exp2(top - peak), axis=0, keepdims=True)
    marginal = peak * LN2 + jnp.log(mass) + base_ref[...]

    largest = jnp.max(marginal, axis=1, keepdims=True)
    scaled = jnp.sum(jnp.exp(marginal - largest), axis=1, keepdims=True)
    lane = lax.broadcasted_iota(jnp.int32, (1, LANES), 1)
    stats[me] = jnp.where(lane < LANES // 2, largest, scaled)
    margs[my_bin] = marginal

    def stat_copy(slot, dev):
        return pltpu.make_async_remote_copy(
            src_ref=stats.at[slot], dst_ref=stats.at[slot], send_sem=send2.at[dev], recv_sem=recv2.at[slot],
            device_id={"draw": dev // n_bin, "bin": lax.rem(dev, n_bin)}, device_id_type=pl.DeviceIdType.MESH)

    def marg_copy(slot, dev):
        return pltpu.make_async_remote_copy(
            src_ref=margs.at[slot], dst_ref=margs.at[slot], send_sem=send3.at[dev], recv_sem=recv3.at[slot],
            device_id={"draw": my_draw, "bin": dev}, device_id_type=pl.DeviceIdType.MESH)

    each(n_all - 1, lambda r: stat_copy(me, lax.rem(me + 1 + r, n_all)).start())
    each(n_bin - 1, lambda r: marg_copy(my_bin, lax.rem(my_bin + 1 + r, n_bin)).start())
    each(n_all - 1, lambda r: stat_copy(lax.rem(me + 1 + r, n_all), me).wait_recv())

    tops = [stats[i] for i in range(n_all)]
    whole_top = functools.reduce(jnp.maximum, tops)
    whole = functools.reduce(jnp.add, [pltpu.roll(x, LANES // 2, 1) * jnp.exp(x - whole_top) for x in tops])
    total_log = (whole_top + jnp.log(whole))[:, 0:1]
    out_ref[:, n_bin * half:] = jnp.broadcast_to(total_log - math.log(half * n_all), (1, LANES))
    each(n_bin - 1, lambda r: marg_copy(lax.rem(my_bin + 1 + r, n_bin), my_bin).wait_recv())
    for q in range(n_bin):
        out_ref[:, q * half:(q + 1) * half] = margs[q] - total_log

    each(n_draw - 1, lambda r: sum_copy(my_draw, lax.rem(my_draw + 1 + r, n_draw)).wait_send())
    each(n_all - 1, lambda r: stat_copy(me, lax.rem(me + 1 + r, n_all)).wait_send())
    each(n_bin - 1, lambda r: marg_copy(my_bin, lax.rem(my_bin + 1 + r, n_bin)).wait_send())


def body(n_draw, n_bin, fine_cross, fine_power, bin_widths, log_amps, delays, phases, chirps, proposal_log):
    dets = fine_power.shape[0]
    bins = bin_widths.shape[0]
    draws = phases.shape[0]
    half = draws // n_bin
    n_all = n_draw * n_bin
    vmem = pl.BlockSpec(memory_space=pltpu.VMEM)
    both = pl.pallas_call(
        functools.partial(kernel, n_draw, n_bin),
        out_shape=pltpu.VMEM((1, draws + LANES), F32),
        in_specs=[pl.BlockSpec(memory_space=pltpu.HBM)] * 8,
        out_specs=vmem,
        scratch_shapes=[
            pltpu.VMEM(fine_cross.shape, F32),
            pltpu.VMEM(fine_power.shape, F32),
            pltpu.VMEM((1, bins), jnp.int32),
            pltpu.VMEM(log_amps.shape, F32),
            pltpu.VMEM(delays.shape, F32),
            pltpu.VMEM((1, draws), F32),
            pltpu.VMEM((1, draws), F32),
            pltpu.VMEM((1, draws), F32),
            pltpu.VMEM((n_draw, 3 * dets + 1, bins), F32),
            pltpu.VMEM((n_all, 1, LANES), F32),
            pltpu.VMEM((n_bin, 1, half), F32),
            pltpu.VMEM((TSHIFT // 2, 4 * bins), BF16),
            pltpu.VMEM((TSHIFT // 2, 4 * bins), BF16),
            pltpu.VMEM((dets, bins, half), F32),
            pltpu.VMEM((dets, bins, half), F32),
            pltpu.VMEM((dets, bins, half), F32),
            pltpu.VMEM((4 * bins, half), BF16),
            pltpu.VMEM((4 * bins, half), BF16),
            pltpu.VMEM((bins, LANES), F32),
            pltpu.VMEM((bins, LANES), F32),
            pltpu.VMEM((1, half), F32),
            pltpu.SemaphoreType.DMA((8,)),
            pltpu.SemaphoreType.DMA((n_draw,)),
            pltpu.SemaphoreType.DMA((n_draw,)),
            pltpu.SemaphoreType.DMA((n_all,)),
            pltpu.SemaphoreType.DMA((n_all,)),
            pltpu.SemaphoreType.DMA((n_bin,)),
            pltpu.SemaphoreType.DMA((n_bin,)),
        ],
        compiler_params=pltpu.CompilerParams(collective_id=0, has_side_effects=True),
        name="evidence",
    )(fine_cross, fine_power, bin_widths.reshape(1, bins), log_amps, delays, phases.reshape(1, draws),
      chirps.reshape(1, draws), proposal_log.reshape(1, draws))
    return both[0, :draws], both[0, draws:draws + 1]


def solution(mesh):
    placed = (
        P("event", None, "draw"),
        P("event", "draw"),
        P("event"),
        P("event", "draw"),
        P("event", "draw"),
        P(("event", "draw")),
        P(("event", "draw")),
        P(("event", "draw")),
    )
    return jax.shard_map(
        functools.partial(body, mesh.shape["draw"], mesh.shape["bin"]),
        mesh=mesh,
        in_specs=placed,
        out_specs=(P(("event", "draw")), P("event")),
        check_vma=False,
    )
```
